32 devices in a mesh: dp: 8 (over y, x, core), tensor: 4 (over z).
Axes of the slice: x: 2, y: 2, z: 4, core: 2. Of those that a mesh axis runs over, the one named last changes fastest.
Arguments:
- text: bfloat16 [8, 256, 5120], P('dp', None, 'tensor'), may hold values from -6 to 6
- prompts: bfloat16 [8, 100, 5120], P('dp', None, 'tensor'), may hold values from -6 to 6
- gain: float32 [5120], replicated, may hold values from 0.1 to 1.9
- w_query: bfloat16 [5120, 3072], P(None, 'tensor'), may hold values from -0.069877124 to 0.069877124, as said below
- w_key: bfloat16 [5120, 3072], P(None, 'tensor'), may hold values from -1.2577882 to 1.2577882, as said below
- w_value: bfloat16 [5120, 3072], P(None, 'tensor'), may hold values from -0.078125 to 0.078125
- cotangent: bfloat16 [8, 356, 3072], P('dp', None, 'tensor'), may hold values from -6 to 6
- task_of: int32 [8], replicated, may hold values from 0 to 7, as said below
- lengths: int32 [8], replicated, may hold values from 1 to 256, as said below
- slot: int32 [8], replicated, may hold values from 0 to 7, as said below
Outputs:
- attn_out: bfloat16 [8, 356, 3072], P('dp', None, 'tensor')
- prompt_grad: float32 [8, 100, 5120], P('dp', None, 'tensor')
The draws below stay inside these ranges and needn't reach their ends.
Inputs may be any that keep to these rules, and one draw needn't show every extreme that they name: `task_of`: nondecreasing along the source order. `lengths`: some example has exactly 256 text tokens; rows of an example beyond its length are padding. `slot`: a permutation of 0 to 7; position s lies on index s // 1 of dp. `w_query`: entries of order 5120 ** -0.5. `w_key`: entries of order 5120 ** -0.5 or larger.
All inputs are finite; a program needn't handle non-finite values.
Results may differ from the reference program's by a relative error of at most 0.0082.
Values may be sent and summed in bfloat16 or wider, within the bound.
No kernel may reach another device: no remote copies, remote signals or barrier semaphores. Data moves between devices by JAX's collectives and lax.ppermute only.
A program may use at most 128 MiB of HBM per device.

```python
import math
import jax
import jax.numpy as jnp
from jax import lax

D = 5120
HEADS = 24
HD = 128
P_SIZE = 100
SEQ = 256
EX_DEV = 1
ROWS = 356
EXAMPLES = 8
TASKS = 8


def weight_base(key):
    return jax.random.truncated_normal(jax.random.fold_in(key, 11), -4.0, 4.0, (D, HEADS * HD), jnp.float32) / math.sqrt(D)


def draw_w_query(key, part):
    return weight_base(key).astype(jnp.bfloat16)


def draw_w_key(key, part):
    noise_part = jax.random.truncated_normal(jax.random.fold_in(key, 12), -4.0, 4.0, (D, HEADS * HD), jnp.float32) / math.sqrt(D)
    result = noise_part
    return result.astype(jnp.bfloat16)


def draw_task_of(key, part):
    first_key, second_key, third_key = jax.random.split(jax.random.fold_in(key, 21), 3)
    first_pick = jax.random.randint(first_key, (EXAMPLES,), 0, TASKS)
    second_pick = jax.random.randint(second_key, (EXAMPLES,), 0, TASKS)
    ranked = jnp.minimum(first_pick, second_pick)
    shuffle = jax.random.permutation(third_key, TASKS)
    return jnp.sort(shuffle[ranked]).astype(jnp.int32)


def length_base(key):
    first_key, second_key = jax.random.split(jax.random.fold_in(key, 31))
    raw_lengths = jax.random.randint(first_key, (EXAMPLES,), 1, SEQ + 1)
    longest = jax.random.randint(second_key, (), 0, EXAMPLES)
    return jnp.where(jnp.arange(EXAMPLES) == longest, SEQ, raw_lengths).astype(jnp.int32)


def draw_lengths(key, part):
    return length_base(key)


def draw_slot(key, part):
    length_all = length_base(key)
    device_count = EXAMPLES // EX_DEV
    order = jnp.argsort(-length_all, stable=True)
    ranks = jnp.arange(EXAMPLES, dtype=jnp.int32)
    rounds = ranks // device_count
    column = ranks % device_count
    device = jnp.where(rounds % 2 == 0, column, device_count - 1 - column)
    placed = (device * EX_DEV + rounds).astype(jnp.int32)
    return jnp.zeros((EXAMPLES,), jnp.int32).at[order].set(placed)


def block_scale(key, dims, shards, least, largest):
    level, own = 1.0, jax.random.fold_in(key, 6)
    for dim, shards_of in shards:
        draws = jnp.exp(jax.random.uniform(jax.random.fold_in(own, dim), (shards_of,), jnp.float32, least / len(shards), largest / len(shards)))
        level = level * jnp.repeat(draws, dims[dim] // shards_of).reshape([-1 if axis == dim else 1 for axis in range(len(dims))])
    return level


def scatter_about(stream_key, shape, width, most, cuts=(), held_as=jnp.bfloat16):
    factor_of = block_scale(stream_key, shape, cuts, -0.22, 0.18) if cuts else 1.0
    array = jax.random.normal(stream_key, shape, jnp.float32) * width * factor_of
    return jnp.minimum(jnp.maximum(array, -most), most).astype(held_as)


def setup_inputs(seed: int = 0) -> dict:
    keys = jax.random.split(jax.random.key(seed), 11)
    return {
        "text": scatter_about(keys[0], (EXAMPLES, SEQ, D), 1.0, 6.0, ((0, 8), (2, 4))),
        "prompts": scatter_about(keys[1], (TASKS, P_SIZE, D), 1.0, 6.0, ((0, 8), (2, 4))),
        "gain": jnp.clip(1.0 + 0.18 * jax.random.normal(keys[2], (D,), jnp.float32), 0.1, 1.9),
        "w_query": draw_w_query(jax.random.fold_in(keys[10], 71), 0),
        "w_key": draw_w_key(jax.random.fold_in(keys[10], 71), 0),
        "w_value": scatter_about(keys[5], (D, HEADS * HD), D ** -0.5, 0.078125, ((1, 4),)),
        "cotangent": scatter_about(keys[6], (EXAMPLES, ROWS, HEADS * HD), 1.0, 6.0, ((0, 8), (2, 4))),
        "task_of": draw_task_of(jax.random.fold_in(keys[10], 71), 0),
        "lengths": draw_lengths(jax.random.fold_in(keys[10], 71), 0),
        "slot": draw_slot(jax.random.fold_in(keys[10], 71), 0),
    }


def rope_tables(row_count):
    half_dim = HD // 2
    frequency = 10000.0 ** (-jnp.arange(half_dim, dtype=jnp.float32) / half_dim)
    angle_table = jnp.arange(row_count, dtype=jnp.float32)[:, None] * frequency[None, :]
    return (jnp.cos(angle_table), jnp.sin(angle_table))

def rotate(vectors, cosine_table, sine_table):
    half_dim = vectors.shape[-1] // 2
    first_half = vectors[..., :half_dim]
    second_half = vectors[..., half_dim:]
    cosine_b = cosine_table[:, None, :]
    sine_b = sine_table[:, None, :]
    return jnp.concatenate([first_half * cosine_b - second_half * sine_b, second_half * cosine_b + first_half * sine_b], axis=-1)

def unrotate(vectors, cosine_table, sine_table):
    half_dim = vectors.shape[-1] // 2
    first_half = vectors[..., :half_dim]
    second_half = vectors[..., half_dim:]
    cosine_b = cosine_table[:, None, :]
    sine_b = sine_table[:, None, :]
    return jnp.concatenate([first_half * cosine_b + second_half * sine_b, second_half * cosine_b - first_half * sine_b], axis=-1)

def transpose_product(grad_low, matrix):
    return lax.dot_general(grad_low, matrix, (((1,), (1,)), ((), ())), preferred_element_type=jnp.float32)

def attention_window(full_rows, gain, w_query, w_key, w_value, cotangent, valid_rows, prompt_len):
    batch_size, row_count, model_width = full_rows.shape
    head_count = w_query.shape[1] // HD
    wide_rows = full_rows.astype(jnp.float32)
    inv_rms = lax.rsqrt(lax.optimization_barrier(jnp.mean(wide_rows * wide_rows, axis=-1)) + 1e-05)
    normed = (wide_rows * inv_rms[..., None] * gain).astype(jnp.bfloat16).reshape(batch_size * row_count, model_width)
    cosine_table, sine_table = rope_tables(row_count)

    def project(matrix):
        return jnp.dot(normed, matrix, preferred_element_type=jnp.float32).reshape(batch_size, row_count, head_count, HD)
    queries = rotate(project(w_query), cosine_table, sine_table).astype(jnp.bfloat16)
    key_rows = rotate(project(w_key), cosine_table, sine_table).astype(jnp.bfloat16)
    value_rows = project(w_value).astype(jnp.bfloat16)
    score_scale = 1.0 / math.sqrt(HD)
    scores = jnp.einsum('erhd,ekhd->ehrk', queries.astype(jnp.float32), key_rows.astype(jnp.float32)) * score_scale
    rows_at = jnp.arange(row_count, dtype=jnp.int32)
    row_limit = (prompt_len + valid_rows).astype(jnp.int32)
    allowed = (rows_at[None, None, :] <= rows_at[None, :, None]) & (rows_at[None, None, :] < row_limit[:, None, None])
    allowed = allowed[:, None]
    scores = jnp.where(allowed, scores, -1e+30)
    row_peak = lax.optimization_barrier(jnp.max(scores, axis=-1, keepdims=True))
    weights = jnp.where(allowed, jnp.exp(scores - row_peak), 0.0)
    probability = weights / lax.optimization_barrier(jnp.sum(weights, axis=-1, keepdims=True))
    probs_low = probability.astype(jnp.bfloat16)
    live_rows = rows_at[None, :] < row_limit[:, None]
    mixed_rows = jnp.einsum('ehrk,ekhd->erhd', probs_low.astype(jnp.float32), value_rows.astype(jnp.float32))
    mixed_rows = jnp.where(live_rows[:, :, None, None], mixed_rows, 0.0)
    output = mixed_rows.reshape(batch_size, row_count, head_count * HD).astype(jnp.bfloat16)
    upstream = jnp.where(live_rows[:, :, None, None], cotangent.reshape(batch_size, row_count, head_count, HD), 0.0).astype(jnp.bfloat16)
    grad_prob = jnp.einsum('erhd,ekhd->ehrk', upstream.astype(jnp.float32), value_rows.astype(jnp.float32))
    row_delta = lax.optimization_barrier(jnp.sum(probability * grad_prob, axis=-1, keepdims=True))
    grad_score = (probability * (grad_prob - row_delta)).astype(jnp.bfloat16)
    grad_query = jnp.einsum('ehrk,ekhd->erhd', grad_score[:, :, :prompt_len, :].astype(jnp.float32), key_rows.astype(jnp.float32)) * score_scale
    grad_key = jnp.einsum('ehrk,erhd->ekhd', grad_score[:, :, :, :prompt_len].astype(jnp.float32), queries.astype(jnp.float32)) * score_scale
    grad_value = jnp.einsum('ehrk,erhd->ekhd', probs_low[:, :, :, :prompt_len].astype(jnp.float32), upstream.astype(jnp.float32))
    cosine_lead = cosine_table[:prompt_len]
    sine_lead = sine_table[:prompt_len]
    flat_rows = batch_size * prompt_len
    grad_query = unrotate(grad_query, cosine_lead, sine_lead).astype(jnp.bfloat16).reshape(flat_rows, head_count * HD)
    grad_key = unrotate(grad_key, cosine_lead, sine_lead).astype(jnp.bfloat16).reshape(flat_rows, head_count * HD)
    grad_value = grad_value.astype(jnp.bfloat16).reshape(flat_rows, head_count * HD)
    grad_normed = transpose_product(grad_query, w_query) + transpose_product(grad_key, w_key) + transpose_product(grad_value, w_value)
    grad_normed = grad_normed.reshape(batch_size, prompt_len, model_width) * gain
    prompt_rows = wide_rows[:, :prompt_len]
    prompt_inv = inv_rms[:, :prompt_len, None]
    grad_rows = prompt_inv * grad_normed - prompt_rows * prompt_inv ** 3 * lax.optimization_barrier(jnp.mean(grad_normed * prompt_rows, axis=-1, keepdims=True))
    return (output, grad_rows)

def reference(text, prompts, gain, w_query, w_key, w_value, cotangent, task_of, lengths, slot):
    example_count = text.shape[0]
    positions = jnp.arange(example_count, dtype=jnp.int32)

    def one_slot(task_grads, place_id):
        hit_mask = slot == place_id
        source = jnp.sum(jnp.where(hit_mask, positions, 0)).astype(jnp.int32)
        task_id = jnp.sum(jnp.where(hit_mask, task_of, 0)).astype(jnp.int32)
        length = jnp.sum(jnp.where(hit_mask, lengths, 0)).astype(jnp.int32)
        joined = jnp.concatenate([prompts[task_id], text[source]], axis=0)[None]
        output, grad_rows = attention_window(joined, gain, w_query, w_key, w_value, cotangent[place_id][None], length[None], P_SIZE)
        task_grads = task_grads.at[task_id].add(grad_rows[0])
        return (task_grads, output[0])
    prompt_grad, attn_out = lax.scan(one_slot, jnp.zeros((TASKS, P_SIZE, D), jnp.float32), positions)
    return (attn_out, prompt_grad)
```

```python
import functools
import math

import jax
import jax.numpy as jnp
from jax import lax
from jax.experimental import pallas as pl
from jax.experimental.pallas import tpu as pltpu
from jax.sharding import PartitionSpec as P

HD = 128
BF16, F32 = jnp.bfloat16, jnp.float32
VM = pl.BlockSpec(memory_space=pltpu.VMEM)
SM = pl.BlockSpec(memory_space=pltpu.SMEM)
ANY = pl.BlockSpec(memory_space=pl.ANY)
PAIR = 2


def up_to(value, step):
    return -(-value // step) * step


def call(body, name, outs, in_specs, args, scratch=(), flops=0, limit=None):
    return pl.pallas_call(
        body,
        name=name,
        out_shape=[jax.ShapeDtypeStruct(s, d) for s, d in outs],
        in_specs=in_specs,
        out_specs=[VM] * len(outs),
        scratch_shapes=list(scratch),
        cost_estimate=pl.CostEstimate(flops=flops, bytes_accessed=1 << 20, transcendentals=0),
        compiler_params=pltpu.CompilerParams(vmem_limit_bytes=limit),
    )(*args)


def partner(me, k, count):
    return me ^ k if count & (count - 1) == 0 else lax.rem(me + k, count)


def group_pairs(count, k):
    pairs = []
    for g in range(count):
        to = g ^ k if count & (count - 1) == 0 else (g + k) % count
        pairs += [(g * PAIR + c, to * PAIR + c) for c in range(PAIR)]
    return pairs


def came_from(me, k, count):
    return me ^ k if count & (count - 1) == 0 else lax.rem(me + count - k, count)


def step_of(source, me, count):
    return source ^ me if count & (count - 1) == 0 else lax.rem(me + count - source, count)


def to_groups(blocks):
    count = len(blocks)
    order = [0] + sorted(range(1, count), key=lambda k: -bin(k).count("1"))
    got = [None] * count
    for k in order:
        got[k] = lax.ppermute(blocks[k], "dp", group_pairs(count, k)) if k else blocks[0]
    return got


def to_sibling(block):
    count = lax.axis_size("dp")
    return lax.ppermute(block, "dp", [(i, i ^ 1) for i in range(count)])


def split_body(count, rows, x_ref, *refs):
    outs, whole = refs[:count], refs[count]
    q = outs[0].shape[0]
    if rows < count * q:
        whole[...] = jnp.zeros_like(whole)
    whole[:rows, :] = x_ref[0]
    me = lax.axis_index("dp") // PAIR
    for k in range(count):
        p = partner(me, k, count)
        outs[k][...] = whole[pl.ds(pl.multiple_of(p * q, q), q), :]


def split_rows(x, count, q, name):
    rows, width = x.shape[1:]
    return call(
        functools.partial(split_body, count, rows),
        name,
        [((q, width), BF16)] * count,
        [VM],
        [x],
        [pltpu.VMEM((count * q, width), BF16)],
    )


def find(slot, values, place, count):
    found = jnp.int32(0)
    for e in range(count):
        found = jnp.where(slot[e] == place, e if values is None else values[e], found)
    return found


def choose_body(count, examples, by_task, slot, task_of, *refs):
    own, sib, outs = refs[:count], refs[count : 2 * count], refs[2 * count : 3 * count]
    held = refs[3 * count]
    index = lax.axis_index("dp")
    me, core = index // PAIR, lax.rem(index, PAIR)
    for k in range(count):
        held[k] = own[k][...]
        held[count + k] = sib[k][...]
    for k in range(count):
        place = partner(me, k, count) * PAIR + core
        e = find(slot, task_of if by_task else None, place, examples)
        at = step_of(e // PAIR, me, count) + jnp.where(lax.rem(e, PAIR) == core, 0, count)
        outs[k][...] = held[at]


def place_rows(pieces, slot, task_of, by_task, name):
    count = len(pieces)
    q, width = pieces[0].shape
    got = to_groups(pieces)
    sib = [to_sibling(b) for b in got]
    chosen = call(
        functools.partial(choose_body, count, slot.shape[0], by_task),
        name,
        [((q, width), BF16)] * count,
        [SM, SM] + [VM] * (2 * count),
        [slot, task_of, *got, *sib],
        [pltpu.VMEM((2 * count, q, width), BF16)],
    )
    return to_groups(chosen)


def join_body(count, parts, rows, *refs):
    ins, outs, whole = refs[:count], refs[count : count + parts], refs[count + parts]
    q = ins[0].shape[0]
    me = lax.axis_index("dp") // PAIR
    for k in range(count):
        p = came_from(me, k, count)
        whole[pl.ds(pl.multiple_of(p * q, q), q), :] = ins[k][...]
    for i in range(parts):
        if outs[i].ndim == 3:
            outs[i][0] = whole[i * rows : (i + 1) * rows, :].astype(outs[i].dtype)
        else:
            outs[i][...] = whole[i * rows : (i + 1) * rows, :].astype(outs[i].dtype)


def join_rows(pieces, parts, rows, name, dtype=BF16, lead=()):
    count = len(pieces)
    q, width = pieces[0].shape
    return call(
        functools.partial(join_body, count, parts, rows),
        name,
        [(lead + (rows, width), dtype)] * parts,
        [VM] * count,
        pieces,
        [pltpu.VMEM((count * q, width), BF16)],
    )


def chain_hops(blocks, axis):
    count = lax.axis_size(axis)
    me = lax.axis_index(axis)
    states = [([b], [b]) for b in blocks]
    for hop in range(1, count):
        right = [(i, i + 1) for i in range(hop - 1, count - 1)]
        left = [(i, i - 1) for i in range(1, count - hop + 1)]
        for from_left, from_right in states:
            if 2 * hop > count + 1:
                here = jnp.where(me >= hop - 1, from_left[-1], from_right[-1])
                both = lax.ppermute(here, axis, right + left)
                from_left.append(both)
                from_right.append(both)
            else:
                from_left.append(lax.ppermute(from_left[-1], axis, right))
                from_right.append(lax.ppermute(from_right[-1], axis, left))
    return states


def spin(x, cosine, sine):
    return x * cosine + pltpu.roll(x, HD // 2, 1) * sine


def nt(a, b):
    return lax.dot_general(a, b, (((1,), (1,)), ((), ())), preferred_element_type=F32)


def tn(a, b):
    return lax.dot_general(a, b, (((0,), (0,)), ((), ())), preferred_element_type=F32)


def chunk_body(cfg, *refs):
    refs = list(refs)

    def take(n):
        out = refs[:n]
        del refs[:n]
        return out

    tp, first, last = cfg["tp"], cfg["first"], cfg["last"]
    rows, lead, lead_pad = cfg["rows"], cfg["lead"], cfg["lead_pad"]
    prompt_len, keys_pad, start = cfg["prompt_len"], cfg["keys_pad"], cfg["start"]
    width, heads, prior = cfg["width"], cfg["heads"], cfg["prior"]
    depth, cols = tp * width, heads * HD
    slot, lengths, gain = take(3)
    weights = take(3)
    cosine, sine, cot = take(3)
    (own,) = take(1)
    from_left = [own] + take(tp - 1)
    from_right = [own] + take(tp - 1)
    before = [take(2) for _ in prior]
    if not first:
        gk_in, gv_in = take(2)
    if last:
        x_lead, inv_lead, gq_lead = take(3)
    (out,) = take(1)
    if last:
        sends = take(tp)
    else:
        k_out, v_out, gk_out, gv_out = take(4)
        if first:
            x_out, inv_out, gq_out = take(3)
    w_buf, sems, x_buf, n_buf, acc, k_all, v_all = take(7)
    if last:
        gk_out, gv_out, gk_low, gv_low, gn_buf = take(5)
    me = lax.axis_index("tensor")

    def weight_copy(m, j):
        rows_of = pl.ds(pl.multiple_of(j * width, width), width)
        return pltpu.make_async_copy(weights[m].at[rows_of], w_buf.at[m, j], sems.at[m, j])

    for j in range(tp):
        for m in range(3):
            weight_copy(m, j).start()
    for j in range(tp):
        for i in range(tp):
            source = own if i == j else from_left[i - j] if i > j else from_right[j - i]

            @pl.when(me == i)
            def _(j=j, source=source):
                x_buf[j] = source[...]

    square = jnp.zeros((rows, 1), F32)
    for j in range(tp):
        wide = x_buf[j].astype(F32)
        square = square + jnp.sum(wide * wide, axis=1, keepdims=True)
    inv_rms = lax.rsqrt(square / depth + 1e-05)
    for j in range(tp):
        n_buf[j] = (x_buf[j].astype(F32) * inv_rms * gain[j]).astype(BF16)
    if first:
        x_out[...] = x_buf[...]
        inv_out[...] = jnp.broadcast_to(inv_rms, (rows, HD))
    acc[...] = jnp.zeros_like(acc)

    def project(j, _):
        for m in range(3):
            weight_copy(m, j).wait()
            acc[m] += jnp.dot(n_buf[j], w_buf[m, j], preferred_element_type=F32)
        return 0

    lax.fori_loop(0, tp, project, 0)
    length = find(slot, lengths, lax.axis_index("dp"), cfg["examples"])
    limit = lead + length
    at = 0
    for (k_ref, v_ref), n in zip(before, prior):
        k_all[at : at + n, :] = k_ref[...]
        v_all[at : at + n, :] = v_ref[...]
        at += n
    if keys_pad > at + rows:
        k_all[at + rows :, :] = jnp.zeros((keys_pad - at - rows, cols), BF16)
        v_all[at + rows :, :] = jnp.zeros((keys_pad - at - rows, cols), BF16)
    cos, sin = cosine[start : start + rows, :], sine[start : start + rows, :]
    scale = 1.0 / math.sqrt(HD)
    r = lax.broadcasted_iota(jnp.int32, (rows, keys_pad), 0) + start
    c = lax.broadcasted_iota(jnp.int32, (rows, keys_pad), 1)
    allowed = (c <= r) & ((c < prompt_len) | (c >= lead)) & (c < limit)
    live = lax.broadcasted_iota(jnp.int32, (rows, HD), 0) + start < limit
    for h in range(heads):
        s = slice(h * HD, (h + 1) * HD)
        q = spin(acc[0, :, s], cos, sin).astype(BF16)
        k_all[at : at + rows, s] = spin(acc[1, :, s], cos, sin).astype(BF16)
        v_all[at : at + rows, s] = acc[2, :, s].astype(BF16)
        k, v = k_all[:, s], v_all[:, s]
        scores = jnp.where(allowed, nt(q, k) * scale, -1e30)
        peak = jnp.max(scores, axis=1, keepdims=True)
        w = jnp.where(allowed, jnp.exp(scores - peak), 0.0)
        prob = w / jnp.sum(w, axis=1, keepdims=True)
        low = prob.astype(BF16)
        mixed = jnp.dot(low, v, preferred_element_type=F32)
        out[:, s] = jnp.where(live, mixed, 0.0).astype(BF16)
        up = jnp.where(live, cot[:, s].astype(F32), 0.0).astype(BF16)
        grad_prob = nt(up, v)
        delta = jnp.sum(prob * grad_prob, axis=1, keepdims=True)
        score = (prob * (grad_prob - delta)).astype(BF16)
        gk = tn(score[:, :lead_pad], q)
        gv = tn(low[:, :lead_pad], up)
        if first:
            gk_out[:, s] = gk
            gv_out[:, s] = gv
            gq = jnp.dot(score, k, preferred_element_type=F32) * scale
            gq_out[:, s] = spin(gq, cos, -sin).astype(BF16)
        else:
            gk_out[:, s] = gk_in[:, s] + gk
            gv_out[:, s] = gv_in[:, s] + gv
    if not last:
        k_out[...] = k_all[at : at + rows, :]
        v_out[...] = v_all[at : at + rows, :]
        return
    cos, sin = cosine[:lead, :], sine[:lead, :]
    for h in range(heads):
        s = slice(h * HD, (h + 1) * HD)
        gk_low[:, s] = spin(gk_out[:lead, s] * scale, cos, -sin).astype(BF16)
        gv_low[:, s] = gv_out[:lead, s].astype(BF16)

    def back(j, total):
        gn = nt(gq_lead[...], w_buf[0, j]) + nt(gk_low[...], w_buf[1, j])
        gn = (gn + nt(gv_low[...], w_buf[2, j])) * gain[j]
        gn_buf[j] = gn
        return total + jnp.sum(gn * x_lead[j].astype(F32), axis=1, keepdims=True)

    total = lax.fori_loop(0, tp, back, jnp.zeros((lead, 1), F32))
    inv = inv_lead[:, :1]
    pull = inv * inv * inv * (total / depth)
    for k in range(tp):
        to = partner(me, k, tp)
        sends[k][...] = (inv * gn_buf[to] - x_lead[to].astype(F32) * pull).astype(BF16)


def sum_body(count, n, *refs):
    ins, outs, whole = refs[:n], refs[n : n + count], refs[n + count]
    rows, q = ins[0].shape[0], outs[0].shape[0]
    total = ins[0][...].astype(F32)
    for i in range(1, n):
        total = total + ins[i][...].astype(F32)
    if rows < count * q:
        whole[rows:, :] = jnp.zeros((count * q - rows, whole.shape[1]), BF16)
    whole[:rows, :] = total.astype(BF16)
    me = lax.axis_index("dp") // PAIR
    for k in range(count):
        p = partner(me, k, count)
        outs[k][...] = whole[pl.ds(pl.multiple_of(p * q, q), q), :]


def collect_body(count, examples, slot, task_of, *refs):
    ins, mine, other = refs[:count], refs[count], refs[count + 1]
    index = lax.axis_index("dp")
    me, core = index // PAIR, lax.rem(index, PAIR)
    tasks = []
    for k in range(count):
        place = came_from(me, k, count) * PAIR + core
        tasks.append(find(slot, task_of, place, examples))
    for g in range(count):
        for target, side in ((mine, core), (other, 1 - core)):
            total = jnp.zeros(ins[0].shape, F32)
            for k in range(count):
                share = jnp.where(tasks[k] == g * PAIR + side, 1.0, 0.0)
                total = total + share * ins[k][...].astype(F32)
            target[g] = total.astype(target.dtype)


def finish_body(count, mine, other, *outs):
    me = lax.axis_index("dp") // PAIR
    for k in range(count):
        p = partner(me, k, count)
        outs[k][...] = (mine[p] + other[p].astype(F32)).astype(BF16)


def on_device(text, prompts, gain, w_query, w_key, w_value, cotangent, task_of, lengths, slot):
    count = lax.axis_size("dp") // PAIR
    tp = lax.axis_size("tensor")
    prompt_len, text_len, width = prompts.shape[1], text.shape[1], text.shape[2]
    examples = slot.shape[0]
    cols = w_query.shape[1]
    heads = cols // HD
    lead = up_to(prompt_len, 16)
    lead_pad = up_to(lead, 128)
    half = text_len // 2
    prompt_q = up_to(-(-prompt_len // count), 16)
    text_q = text_len // count
    pieces_a = split_rows(prompts, count, prompt_q, "split_prompt")
    pieces_b = split_rows(text, count, text_q, "split_text")
    placed_a = place_rows(pieces_a, slot, task_of, True, "choose_prompt")
    placed_b = place_rows(pieces_b, slot, task_of, False, "choose_text")
    (rows_a,) = join_rows(placed_a, 1, lead, "join_prompt")
    rows_b, rows_c = join_rows(placed_b, 2, half, "join_text")
    states = chain_hops([rows_a, rows_b, rows_c], "tensor")

    at = jnp.arange(lead + text_len, dtype=jnp.int32)
    at = jnp.where(at < lead, at, at - (lead - prompt_len)).astype(F32)
    frequency = 10000.0 ** (-jnp.arange(HD // 2, dtype=F32) / (HD // 2))
    angle = at[:, None] * frequency[None, :]
    cosine, sine = jnp.cos(angle), jnp.sin(angle)
    cosine = jnp.concatenate([cosine, cosine], axis=1)
    sine = jnp.concatenate([-sine, sine], axis=1)
    gain_rows = gain.reshape(tp, 1, width)
    cots = [
        jnp.pad(cotangent[0, :prompt_len], ((0, lead - prompt_len), (0, 0))),
        cotangent[0, prompt_len : prompt_len + half],
        cotangent[0, prompt_len + half :],
    ]
    outputs, before, grads, saved = [], [], [], []
    for i, (from_left, from_right) in enumerate(states):
        first, last = i == 0, i == len(states) - 1
        rows = cots[i].shape[0]
        start = 0 if first else lead + (i - 1) * half
        keys_pad = up_to(start + rows, 128)
        cfg = dict(
            tp=tp, first=first, last=last, rows=rows, lead=lead, lead_pad=lead_pad,
            prompt_len=prompt_len, keys_pad=keys_pad, start=start, width=width, heads=heads,
            prior=[k.shape[0] for k, _ in before], examples=examples,
        )
        args = [slot, lengths, gain_rows, w_query, w_key, w_value, cosine, sine, cots[i]]
        specs = [SM, SM, VM, ANY, ANY, ANY, VM, VM, VM]
        extra = [from_left[0], *from_left[1:], *from_right[1:]]
        for pair in before:
            extra += pair
        extra += grads + (saved if last else [])
        outs = [((rows, cols), BF16)]
        scratch = [
            pltpu.VMEM((3, tp, width, cols), BF16),
            pltpu.SemaphoreType.DMA((3, tp)),
            pltpu.VMEM((tp, rows, width), BF16),
            pltpu.VMEM((tp, rows, width), BF16),
            pltpu.VMEM((3, rows, cols), F32),
            pltpu.VMEM((keys_pad, cols), BF16),
            pltpu.VMEM((keys_pad, cols), BF16),
        ]
        if last:
            outs += [((lead, width), BF16)] * tp
            scratch += [pltpu.VMEM((lead_pad, cols), F32)] * 2
            scratch += [pltpu.VMEM((lead, cols), BF16)] * 2
            scratch += [pltpu.VMEM((tp, lead, width), F32)]
        else:
            outs += [((rows, cols), BF16)] * 2 + [((lead_pad, cols), F32)] * 2
            if first:
                outs += [((tp, rows, width), BF16), ((rows, HD), F32), ((rows, cols), BF16)]
        got = call(
            functools.partial(chunk_body, cfg),
            "rows_%d" % i,
            outs,
            specs + [VM] * len(extra),
            args + extra,
            scratch,
            flops=2 * rows * tp * width * 3 * cols,
        )
        outputs.append(got[0])
        if last:
            sends = got[1:]
        else:
            before.append((got[1], got[2]))
            grads = [got[3], got[4]]
            if first:
                saved = list(got[5:])
    output = jnp.concatenate([outputs[0][:prompt_len], *outputs[1:]], axis=0)[None]

    got = [sends[0]]
    for k in sorted(range(1, tp), reverse=True):
        pairs = [(i, i ^ k if tp & (tp - 1) == 0 else (i + k) % tp) for i in range(tp)]
        got.append(lax.ppermute(sends[k], "tensor", pairs))
    pieces = call(
        functools.partial(sum_body, count, tp),
        "sum_heads",
        [((prompt_q, width), BF16)] * count,
        [VM] * tp,
        got,
        [pltpu.VMEM((count * prompt_q, width), BF16)],
    )
    mine, other = call(
        functools.partial(collect_body, count, examples),
        "collect",
        [((count, prompt_q, width), F32), ((count, prompt_q, width), BF16)],
        [SM, SM] + [VM] * count,
        [slot, task_of, *to_groups(pieces)],
    )
    done = call(
        functools.partial(finish_body, count),
        "finish",
        [((prompt_q, width), BF16)] * count,
        [VM, VM],
        [mine, to_sibling(other)],
    )
    (prompt_grad,) = join_rows(to_groups(done), 1, prompt_len, "join_grad", F32, (1,))
    return (output, prompt_grad)


def solution(mesh):
    in_specs = (
        P("dp", None, "tensor"),
        P("dp", None, "tensor"),
        P(),
        P(None, "tensor"),
        P(None, "tensor"),
        P(None, "tensor"),
        P("dp", None, "tensor"),
        P(),
        P(),
        P(),
    )
    out_specs = (P("dp", None, "tensor"), P("dp", None, "tensor"))
    return jax.shard_map(
        on_device, mesh=mesh, in_specs=in_specs, out_specs=out_specs, check_vma=False
    )
```

```python
import functools
import math

import jax
import jax.numpy as jnp
from jax import lax
from jax.experimental import pallas as pl
from jax.experimental.pallas import tpu as pltpu
from jax.sharding import PartitionSpec as P


HD = 128
BF16, F32 = jnp.bfloat16, jnp.float32
VM = pl.BlockSpec(memory_space=pltpu.VMEM)
SM = pl.BlockSpec(memory_space=pltpu.SMEM)
ANY = pl.BlockSpec(memory_space=pl.ANY)
PAIR = 2
LIMIT = 16 << 20
WAIT = 10**9


def up_to(value, step):
    return -(-value // step) * step


def call(body, outs, in_specs, args, scratch=(), flops=WAIT, limit=LIMIT):
    return pl.pallas_call(
        body,
        out_shape=[jax.ShapeDtypeStruct(s, d) for s, d in outs],
        in_specs=in_specs,
        out_specs=[VM] * len(outs),
        scratch_shapes=list(scratch),
        cost_estimate=pl.CostEstimate(flops=flops, bytes_accessed=1 << 20, transcendentals=0),
        compiler_params=pltpu.CompilerParams(vmem_limit_bytes=limit),
    )(*args)


def partner(me, k, count):
    return me ^ k if count & (count - 1) == 0 else lax.rem(me + k, count)


def group_pairs(count, k):
    pairs = []
    for g in range(count):
        to = g ^ k if count & (count - 1) == 0 else (g + k) % count
        pairs += [(g * PAIR + c, to * PAIR + c) for c in range(PAIR)]
    return pairs


def came_from(me, k, count):
    return me ^ k if count & (count - 1) == 0 else lax.rem(me + count - k, count)


def step_of(source, me, count):
    return source ^ me if count & (count - 1) == 0 else lax.rem(me + count - source, count)


def far_first(count):
    return sorted(range(1, count), key=lambda k: -bin(k).count("1"))


def to_groups(blocks):
    count = len(blocks)
    got = [blocks[0]] + [None] * (count - 1)
    for k in far_first(count):
        got[k] = lax.ppermute(blocks[k], "dp", group_pairs(count, k))
    return got


def to_sibling(block):
    count = lax.axis_size("dp")
    return lax.ppermute(block, "dp", [(i, i ^ 1) for i in range(count)])


def split_body(count, q_lead, skip, p_ref, x_ref, *refs):
    outs, held = refs[:count], refs[count]
    n_lead = p_ref.shape[1]
    q = held.shape[1] - q_lead
    for g in range(count):
        n = max(0, min(q_lead, n_lead - g * q_lead))
        if n < q_lead:
            held[g] = jnp.zeros(held.shape[1:], BF16)
        if n:
            held[g, :n, :] = p_ref[0, g * q_lead : g * q_lead + n, :]
        held[g, q_lead:, :] = x_ref[0, skip + g * q : skip + (g + 1) * q, :]
    me = lax.axis_index("dp") // PAIR
    for k in range(count):
        outs[k][...] = held[partner(me, k, count)]


def spread_body(count, tp, *refs):
    n = block_count(tp)
    blocks, outs, held = refs[:n], refs[n : n + count], refs[-1]
    q = outs[0].shape[1]
    gather_blocks(tp, blocks, held)
    me = lax.axis_index("dp") // PAIR
    for k in range(count):
        p = partner(me, k, count)
        for g in range(count):

            @pl.when(p == g)
            def _(k=k, g=g):
                outs[k][...] = held[:, g * q : (g + 1) * q, :]


def gather_blocks(tp, blocks, held, at=0):
    rows = blocks[0].shape[0]
    me = lax.axis_index("tensor")
    for j in range(tp):
        for i in range(tp):
            source = blocks[holds(tp, i, j)]

            @pl.when(me == i)
            def _(j=j, source=source):
                held[j, at : at + rows, :] = source[...]


def find(slot, values, place, count):
    found = jnp.int32(0)
    for e in range(count):
        found = jnp.where(slot[e] == place, e if values is None else values[e], found)
    return found


def choose_body(count, examples, q_lead, slot, task_of, *refs):
    own, sib, outs = refs[:count], refs[count : 2 * count], refs[2 * count : 3 * count]
    held = refs[3 * count]
    index = lax.axis_index("dp")
    me, core = index // PAIR, lax.rem(index, PAIR)
    for k in range(count):
        held[k] = own[k][...]
        held[count + k] = sib[k][...]

    def where_is(e):
        return step_of(e // PAIR, me, count) + jnp.where(lax.rem(e, PAIR) == core, 0, count)

    for k in range(count):
        place = partner(me, k, count) * PAIR + core
        at = where_is(find(slot, None, place, examples))
        if q_lead:
            outs[k][q_lead:] = held[at, q_lead:]
            outs[k][:q_lead] = held[where_is(find(slot, task_of, place, examples)), :q_lead]
        else:
            outs[k][...] = held[at]


def place_rows(pieces, slot, task_of, q_lead):
    count = len(pieces)
    shape = pieces[0].shape
    got = to_groups(pieces)
    sib = [to_sibling(b) for b in got]
    chosen = call(
        functools.partial(choose_body, count, slot.shape[0], q_lead),
        [(shape, BF16)] * count,
        [SM, SM] + [VM] * (2 * count),
        [slot, task_of, *got, *sib],
        [pltpu.VMEM((2 * count,) + shape, BF16)],
    )
    return to_groups(chosen)


def join_body(count, cuts, *refs):
    ins, outs, held = refs[:count], refs[count : count + len(cuts)], refs[-1]
    me = lax.axis_index("dp") // PAIR
    for k in range(count):
        held[came_from(me, k, count)] = ins[k][...]
    for out, (low, high, rows) in zip(outs, cuts):
        q = high - low
        for g in range(count):
            n = max(0, min(q, rows - g * q))
            if n and len(ins[0].shape) == 3:
                out[:, g * q : g * q + n, :] = held[g, :, low : low + n, :]
            elif n and len(out.shape) == 3:
                out[0, g * q : g * q + n, :] = held[g, low : low + n, :].astype(out.dtype)
            elif n:
                out[g * q : g * q + n, :] = held[g, low : low + n, :].astype(out.dtype)


def join_rows(pieces, cuts, dtype=BF16, lead=()):
    count = len(pieces)
    shape = pieces[0].shape
    return call(
        functools.partial(join_body, count, cuts),
        [(lead + (rows, shape[-1]), dtype) for _, _, rows in cuts],
        [VM] * count,
        pieces,
        [pltpu.VMEM((count,) + shape, BF16)],
    )


def holds(tp, i, j):
    if tp != 4:
        return i - j if i >= j else tp - 1 + j - i
    return i ^ j if i ^ j < 3 else 3 + int(i in (0, tp - 1))


def block_count(tp):
    return 5 if tp == 4 else 2 * tp - 1


def chain_gather(block, axis):
    tp = lax.axis_size(axis)

    def move(value, pairs):
        return lax.ppermute(value, axis, pairs)

    if tp == 4:
        far = move(block, [(i, i ^ 2) for i in range(4)])
        pair = move(block, [(i, i ^ 1) for i in range(4)])
        mid = move(block, [(1, 2), (2, 1)])
        passed = move(far, [(1, 0), (2, 3)])
        return [block, pair, far, mid, passed]
    from_left, from_right = [block], [block]
    for hop in range(1, tp):
        right = [(i, i + 1) for i in range(hop - 1, tp - 1)]
        left = [(i, i - 1) for i in range(1, tp - hop + 1)]
        from_left.append(move(from_left[-1], right))
        from_right.append(move(from_right[-1], left))
    return [block, *from_left[1:], *from_right[1:]]


def spin(x, cosine, sine):
    return x * cosine + pltpu.roll(x, HD // 2, 1) * sine


def nt(a, b):
    return lax.dot_general(a, b, (((1,), (1,)), ((), ())), preferred_element_type=F32)


def tn(a, b):
    return lax.dot_general(a, b, (((0,), (0,)), ((), ())), preferred_element_type=F32)


def chunk_body(cfg, *refs):
    refs = list(refs)

    def take(n):
        out = refs[:n]
        del refs[:n]
        return out

    tp, first, last = cfg["tp"], cfg["first"], cfg["last"]
    rows, lead, lead_pad = cfg["rows"], cfg["lead"], cfg["lead_pad"]
    prompt_len, keys_pad, start = cfg["prompt_len"], cfg["keys_pad"], cfg["start"]
    width, heads, prior = cfg["width"], cfg["heads"], cfg["prior"]
    depth, cols = tp * width, heads * HD
    slot, lengths, gain = take(3)
    weights = take(3)
    cosine, sine, cot = take(3)
    segments = [take(block_count(tp) if chained else 1) for chained, _ in cfg["segments"]]
    before = [take(2) for _ in prior]
    if not first:
        gk_in, gv_in = take(2)
    if last:
        inv_lead, flat_lead, dot_lead = take(3)
    (out,) = take(1)
    if last:
        turned, pull_out = take(2)
    else:
        k_out, v_out, gk_out, gv_out = take(4)
        if first:
            x_out, inv_out, flat_out, dot_out, turned = take(5)
    x_buf, n_buf, acc, k_all, v_all = take(5)
    if last:
        gk_out, gv_out = take(2)

    def weight(m, j):
        return weights[m][pl.ds(pl.multiple_of(j * width, width), width), :]

    at = 0
    for blocks, (chained, n) in zip(segments, cfg["segments"]):
        if chained:
            gather_blocks(tp, blocks, x_buf, at)
        else:
            x_buf[:, at : at + n, :] = blocks[0][...]
        at += n
    square = jnp.zeros((rows, 1), F32)
    for j in range(tp):
        wide = x_buf[j].astype(F32)
        square = square + jnp.sum(wide * wide, axis=1, keepdims=True)
    inv_rms = lax.rsqrt(square / depth + 1e-05)
    for j in range(tp):
        n_buf[j] = (x_buf[j].astype(F32) * inv_rms * gain[j]).astype(BF16)
    if first:
        x_out[...] = x_buf[:, :lead, :]
        inv_out[...] = jnp.broadcast_to(inv_rms[:lead], (lead, HD))
    acc[...] = jnp.zeros_like(acc)

    def project(j, _):
        for m in range(3):
            acc[m] += jnp.dot(n_buf[j], weight(m, j), preferred_element_type=F32)
        return 0

    lax.fori_loop(0, tp, project, 0)
    length = find(slot, lengths, lax.axis_index("dp"), cfg["examples"])
    limit = lead + length
    at = 0
    for (k_ref, v_ref), n in zip(before, prior):
        k_all[at : at + n, :] = k_ref[...]
        v_all[at : at + n, :] = v_ref[...]
        at += n
    if keys_pad > at + rows:
        k_all[at + rows :, :] = jnp.zeros((keys_pad - at - rows, cols), BF16)
        v_all[at + rows :, :] = jnp.zeros((keys_pad - at - rows, cols), BF16)
    cos, sin = cosine[start : start + rows, :], sine[start : start + rows, :]
    scale = 1.0 / math.sqrt(HD)
    r = lax.broadcasted_iota(jnp.int32, (rows, keys_pad), 0) + start
    c = lax.broadcasted_iota(jnp.int32, (rows, keys_pad), 1)
    allowed = (c <= r) & ((c < prompt_len) | (c >= lead)) & (c < limit)
    live = lax.broadcasted_iota(jnp.int32, (rows, HD), 0) + start < limit
    dot = jnp.zeros((rows, 1), F32)
    for h in range(heads):
        s = slice(h * HD, (h + 1) * HD)
        q = spin(acc[0, :, s], cos, sin).astype(BF16)
        k_all[at : at + rows, s] = spin(acc[1, :, s], cos, sin).astype(BF16)
        v_all[at : at + rows, s] = acc[2, :, s].astype(BF16)
        k, v = k_all[:, s], v_all[:, s]
        scores = jnp.where(allowed, nt(q, k) * scale, -1e30)
        peak = jnp.max(scores, axis=1, keepdims=True)
        w = jnp.exp(scores - peak)
        prob = w * (1.0 / jnp.sum(w, axis=1, keepdims=True))
        low = prob.astype(BF16)
        mixed = jnp.dot(low, v, preferred_element_type=F32)
        out[:, s] = jnp.where(live, mixed, 0.0).astype(BF16)
        up = jnp.where(live, cot[:, s].astype(F32), 0.0).astype(BF16)
        grad_prob = nt(up, v)
        delta = jnp.sum(prob * grad_prob, axis=1, keepdims=True)
        score = (prob * (grad_prob - delta)).astype(BF16)
        gk = tn(score[:, :lead_pad], q)
        gv = tn(low[:, :lead_pad], up)
        if first:
            gk_out[:, s] = gk
            gv_out[:, s] = gv
            gq = jnp.dot(score, k, preferred_element_type=F32) * scale
            gq = spin(gq, cos, -sin).astype(BF16).astype(F32)
            dot = dot + jnp.sum(gq * acc[0, :, s], axis=1, keepdims=True)
            gq = jnp.concatenate([gq, jnp.zeros((lead_pad - lead, HD), F32)], axis=0)
            turned[s, :] = gq.T.astype(BF16)
        else:
            gk_out[:, s] = gk_in[:, s] + gk
            gv_out[:, s] = gv_in[:, s] + gv
    if first:
        flat_out[...] = acc[1:]
        dot_out[...] = jnp.broadcast_to(dot, (rows, HD))
    if not last:
        k_out[...] = k_all[at : at + rows, :]
        v_out[...] = v_all[at : at + rows, :]
        return
    cos, sin = cosine[:lead_pad, :], sine[:lead_pad, :]
    dot = dot_lead[:, :1]
    for h in range(heads):
        s = slice(h * HD, (h + 1) * HD)
        gk = spin(gk_out[:, s] * scale, cos, -sin).astype(BF16).astype(F32)
        gv = gv_out[:, s].astype(BF16).astype(F32)
        dot = dot + jnp.sum(gk[:lead] * flat_lead[0, :, s], axis=1, keepdims=True)
        dot = dot + jnp.sum(gv[:lead] * flat_lead[1, :, s], axis=1, keepdims=True)
        turned[0, s, :] = gk.T.astype(BF16)
        turned[1, s, :] = gv.T.astype(BF16)
    inv = inv_lead[:, :1]
    pull_out[...] = jnp.broadcast_to(inv * inv * (dot / depth), (lead, HD))


def back_body(tp, k, gain, wq, wk, wv, x_lead, inv_lead, pull, turned_q, turned, out):
    lead, width = out.shape
    to = partner(lax.axis_index("tensor"), k, tp)
    at = pl.ds(pl.multiple_of(to * width, width), width)
    gn = jnp.dot(wq[at, :], turned_q[...], preferred_element_type=F32)
    gn = gn + jnp.dot(wk[at, :], turned[0], preferred_element_type=F32)
    gn = gn + jnp.dot(wv[at, :], turned[1], preferred_element_type=F32)
    gn = gn.T[:lead] * gain[to]
    out[...] = (inv_lead[:, :1] * gn - x_lead[to].astype(F32) * pull[:, :1]).astype(BF16)


def sum_body(count, n, *refs):
    ins, outs, whole, held = refs[:n], refs[n : n + count], refs[n + count], refs[n + count + 1]
    rows, q = ins[0].shape[0], outs[0].shape[0]
    total = ins[0][...].astype(F32)
    for i in range(1, n):
        total = total + ins[i][...].astype(F32)
    whole[...] = total.astype(BF16)
    for g in range(count):
        m = max(0, min(q, rows - g * q))
        if m < q:
            held[g] = jnp.zeros(held.shape[1:], BF16)
        if m:
            held[g, :m, :] = whole[g * q : g * q + m, :]
    me = lax.axis_index("dp") // PAIR
    for k in range(count):
        outs[k][...] = held[partner(me, k, count)]


def collect_body(count, examples, slot, task_of, *refs):
    ins, mine, other = refs[:count], refs[count], refs[count + 1]
    index = lax.axis_index("dp")
    me, core = index // PAIR, lax.rem(index, PAIR)
    tasks = []
    for k in range(count):
        place = came_from(me, k, count) * PAIR + core
        tasks.append(find(slot, task_of, place, examples))
    for g in range(count):
        for target, side in ((mine, core), (other, 1 - core)):
            total = jnp.zeros(ins[0].shape, F32)
            for k in range(count):
                share = jnp.where(tasks[k] == g * PAIR + side, 1.0, 0.0)
                total = total + share * ins[k][...].astype(F32)
            target[g] = total.astype(target.dtype)


def finish_body(count, mine, other, *outs):
    me = lax.axis_index("dp") // PAIR
    for k in range(count):
        p = partner(me, k, count)
        outs[k][...] = (mine[p] + other[p].astype(F32)).astype(BF16)


def on_device(text, prompts, gain, w_query, w_key, w_value, cotangent, task_of, lengths, slot):
    count = lax.axis_size("dp") // PAIR
    tp = lax.axis_size("tensor")
    prompt_len, text_len, width = prompts.shape[1], text.shape[1], text.shape[2]
    examples = slot.shape[0]
    cols = w_query.shape[1]
    heads = cols // HD
    lead = up_to(prompt_len, 8)
    lead_pad = up_to(lead, 128)
    early = text_len // 2
    late = text_len - early
    prompt_q = up_to(-(-prompt_len // count), 16)
    late_q, early_q = late // count, early // count
    wide = chain_gather(text[0, :early], "tensor")
    piece = (prompt_q + late_q, width)
    pieces = call(
        functools.partial(split_body, count, prompt_q, early),
        [(piece, BF16)] * count,
        [VM, VM],
        [prompts, text],
        [pltpu.VMEM((count,) + piece, BF16)],
    )
    placed = place_rows(pieces, slot, task_of, prompt_q)
    cuts = [(0, prompt_q, lead), (prompt_q, prompt_q + late_q, late)]
    rows_a, rows_c = join_rows(placed, cuts)
    chain_a = chain_gather(rows_a, "tensor")
    chain_c = chain_gather(rows_c, "tensor")
    wide_pieces = call(
        functools.partial(spread_body, count, tp),
        [((tp, early_q, width), BF16)] * count,
        [VM] * len(wide),
        wide,
        [pltpu.VMEM((tp, early, width), BF16)],
    )
    wide_placed = place_rows(wide_pieces, slot, task_of, 0)
    (rows_b,) = join_rows(wide_placed, [(0, early_q, early)], BF16, (tp,))

    at = jnp.arange(lead + text_len, dtype=jnp.int32)
    at = jnp.where(at < lead, at, at - (lead - prompt_len)).astype(F32)
    frequency = 10000.0 ** (-jnp.arange(HD // 2, dtype=F32) / (HD // 2))
    angle = at[:, None] * frequency[None, :]
    cosine, sine = jnp.cos(angle), jnp.sin(angle)
    cosine = jnp.concatenate([cosine, cosine], axis=1)
    sine = jnp.concatenate([-sine, sine], axis=1)
    gain_rows = gain.reshape(tp, 1, width)
    split_at = prompt_len + early
    cots = [
        jnp.pad(cotangent[0, :prompt_len], ((0, lead - prompt_len), (0, 0))),
        cotangent[0, prompt_len:split_at],
        cotangent[0, split_at:],
    ]
    chunks = [
        ([(True, lead)], chain_a),
        ([(False, early)], [rows_b]),
        ([(True, late)], chain_c),
    ]
    outputs, before, grads, saved, start = [], [], [], [], 0
    for i, (segments, blocks) in enumerate(chunks):
        first, last = i == 0, i == len(chunks) - 1
        rows = cots[i].shape[0]
        keys_pad = up_to(start + rows, 128)
        cfg = dict(
            tp=tp, first=first, last=last, rows=rows, lead=lead, lead_pad=lead_pad,
            prompt_len=prompt_len, keys_pad=keys_pad, start=start, width=width, heads=heads,
            prior=[k.shape[0] for k, _ in before], examples=examples, segments=segments,
        )
        args = [slot, lengths, gain_rows, w_query, w_key, w_value, cosine, sine, cots[i]]
        specs = [SM, SM] + [VM] * 7
        extra = list(blocks)
        for pair in before:
            extra += pair
        extra += grads + (saved[1:4] if last else [])
        outs = [((rows, cols), BF16)]
        scratch = [
            pltpu.VMEM((tp, rows, width), BF16),
            pltpu.VMEM((tp, rows, width), BF16),
            pltpu.VMEM((3, rows, cols), F32),
            pltpu.VMEM((keys_pad, cols), BF16),
            pltpu.VMEM((keys_pad, cols), BF16),
        ]
        if last:
            outs += [((2, cols, lead_pad), BF16), ((lead, HD), F32)]
            scratch += [pltpu.VMEM((lead_pad, cols), F32)] * 2
        else:
            outs += [((rows, cols), BF16)] * 2 + [((lead_pad, cols), F32)] * 2
            if first:
                outs += [((tp, lead, width), BF16), ((lead, HD), F32), ((2, lead, cols), F32)]
                outs += [((lead, HD), F32), ((cols, lead_pad), BF16)]
        got = call(
            functools.partial(chunk_body, cfg),
            outs,
            specs + [VM] * len(extra),
            args + extra,
            scratch,
            flops=2 * rows * tp * width * 3 * cols,
        )
        outputs.append(got[0])
        if last:
            turned, pull = got[1:]
        else:
            before.append((got[1], got[2]))
            grads = [got[3], got[4]]
            if first:
                saved = list(got[5:])
        start += rows
    output = jnp.concatenate([outputs[0][:prompt_len], *outputs[1:]], axis=0)[None]

    x_lead, inv_lead, _, _, turned_q = saved
    got = []
    for k in reversed(range(tp)):
        (block,) = call(
            functools.partial(back_body, tp, k),
            [((lead, width), BF16)],
            [VM] * 9,
            [gain_rows, w_query, w_key, w_value, x_lead, inv_lead, pull, turned_q, turned],
        )
        if k:
            pairs = [(i, i ^ k if tp & (tp - 1) == 0 else (i + k) % tp) for i in range(tp)]
            block = lax.ppermute(block, "tensor", pairs)
        got.append(block)
    pieces = call(
        functools.partial(sum_body, count, tp),
        [((prompt_q, width), BF16)] * count,
        [VM] * tp,
        got,
        [pltpu.VMEM((lead, width), BF16), pltpu.VMEM((count, prompt_q, width), BF16)],
    )
    mine, other = call(
        functools.partial(collect_body, count, examples),
        [((count, prompt_q, width), F32), ((count, prompt_q, width), BF16)],
        [SM, SM] + [VM] * count,
        [slot, task_of, *to_groups(pieces)],
    )
    done = call(
        functools.partial(finish_body, count),
        [((prompt_q, width), BF16)] * count,
        [VM, VM],
        [mine, to_sibling(other)],
    )
    (prompt_grad,) = join_rows(to_groups(done), [(0, prompt_q, prompt_len)], F32, (1,))
    return (output, prompt_grad)


def solution(mesh):
    in_specs = (
        P("dp", None, "tensor"),
        P("dp", None, "tensor"),
        P(),
        P(None, "tensor"),
        P(None, "tensor"),
        P(None, "tensor"),
        P("dp", None, "tensor"),
        P(),
        P(),
        P(),
    )
    out_specs = (P("dp", None, "tensor"), P("dp", None, "tensor"))
    return jax.shard_map(
        on_device, mesh=mesh, in_specs=in_specs, out_specs=out_specs, check_vma=False
    )
```

```python
import functools
import math

import jax
import jax.numpy as jnp
from jax import lax
from jax.experimental import pallas as pl
from jax.experimental.pallas import tpu as pltpu
from jax.sharding import PartitionSpec as P


HD = 128
BF16, F32 = jnp.bfloat16, jnp.float32
VM = pl.BlockSpec(memory_space=pltpu.VMEM)
SM = pl.BlockSpec(memory_space=pltpu.SMEM)
ANY = pl.BlockSpec(memory_space=pl.ANY)
PAIR = 2
LIMIT = 16 << 20
WAIT = 2 * 10**9


def up_to(value, step):
    return -(-value // step) * step


def call(body, outs, in_specs, args, scratch=(), flops=WAIT, limit=LIMIT):
    return pl.pallas_call(
        body,
        out_shape=[jax.ShapeDtypeStruct(s, d) for s, d in outs],
        in_specs=in_specs,
        out_specs=[VM] * len(outs),
        scratch_shapes=list(scratch),
        cost_estimate=pl.CostEstimate(flops=flops, bytes_accessed=1 << 20, transcendentals=0),
        compiler_params=pltpu.CompilerParams(vmem_limit_bytes=limit),
    )(*args)


def partner(me, k, count):
    return me ^ k if count & (count - 1) == 0 else lax.rem(me + k, count)


def group_pairs(count, k):
    pairs = []
    for g in range(count):
        to = g ^ k if count & (count - 1) == 0 else (g + k) % count
        pairs += [(g * PAIR + c, to * PAIR + c) for c in range(PAIR)]
    return pairs


def came_from(me, k, count):
    return me ^ k if count & (count - 1) == 0 else lax.rem(me + count - k, count)


def step_of(source, me, count):
    return source ^ me if count & (count - 1) == 0 else lax.rem(me + count - source, count)


def far_first(count):
    return sorted(range(1, count), key=lambda k: -bin(k).count("1"))


def to_groups(blocks):
    count = len(blocks)
    got = [blocks[0]] + [None] * (count - 1)
    for k in far_first(count):
        got[k] = lax.ppermute(blocks[k], "dp", group_pairs(count, k))
    return got


def to_sibling(block):
    count = lax.axis_size("dp")
    return lax.ppermute(block, "dp", [(i, i ^ 1) for i in range(count)])


def split_body(count, q_lead, skip, p_ref, x_ref, *refs):
    outs, held = refs[:count], refs[count]
    n_lead = p_ref.shape[1]
    q = held.shape[1] - q_lead
    for g in range(count):
        n = max(0, min(q_lead, n_lead - g * q_lead))
        if n < q_lead:
            held[g] = jnp.zeros(held.shape[1:], BF16)
        if n:
            held[g, :n, :] = p_ref[0, g * q_lead : g * q_lead + n, :]
        held[g, q_lead:, :] = x_ref[0, skip + g * q : skip + (g + 1) * q, :]
    me = lax.axis_index("dp") // PAIR
    for k in range(count):
        outs[k][...] = held[partner(me, k, count)]


def spread_body(count, tp, *refs):
    n = block_count(tp)
    blocks, outs, held = refs[:n], refs[n : n + count], refs[-1]
    q = outs[0].shape[1]
    gather_blocks(tp, blocks, held)
    me = lax.axis_index("dp") // PAIR
    for k in range(count):
        p = partner(me, k, count)
        for g in range(count):

            @pl.when(p == g)
            def _(k=k, g=g):
                outs[k][...] = held[:, g * q : (g + 1) * q, :]


def gather_blocks(tp, blocks, held, at=0):
    rows = blocks[0].shape[0]
    me = lax.axis_index("tensor")
    for j in range(tp):
        for i in range(tp):
            source = blocks[holds(tp, i, j)]

            @pl.when(me == i)
            def _(j=j, source=source):
                held[j, at : at + rows, :] = source[...]


def find(slot, values, place, count):
    found = jnp.int32(0)
    for e in range(count):
        found = jnp.where(slot[e] == place, e if values is None else values[e], found)
    return found


def choose_body(count, examples, q_lead, slot, task_of, *refs):
    own, sib, outs = refs[:count], refs[count : 2 * count], refs[2 * count : 3 * count]
    held = refs[3 * count]
    index = lax.axis_index("dp")
    me, core = index // PAIR, lax.rem(index, PAIR)
    for k in range(count):
        held[k] = own[k][...]
        held[count + k] = sib[k][...]

    def where_is(e):
        return step_of(e // PAIR, me, count) + jnp.where(lax.rem(e, PAIR) == core, 0, count)

    for k in range(count):
        place = partner(me, k, count) * PAIR + core
        at = where_is(find(slot, None, place, examples))
        if q_lead:
            outs[k][q_lead:] = held[at, q_lead:]
            outs[k][:q_lead] = held[where_is(find(slot, task_of, place, examples)), :q_lead]
        else:
            outs[k][...] = held[at]


def place_rows(pieces, slot, task_of, q_lead):
    count = len(pieces)
    shape = pieces[0].shape
    got = to_groups(pieces)
    sib = [to_sibling(b) for b in got]
    chosen = call(
        functools.partial(choose_body, count, slot.shape[0], q_lead),
        [(shape, BF16)] * count,
        [SM, SM] + [VM] * (2 * count),
        [slot, task_of, *got, *sib],
        [pltpu.VMEM((2 * count,) + shape, BF16)],
    )
    return to_groups(chosen)


def join_body(count, cuts, *refs):
    ins, outs, held = refs[:count], refs[count : count + len(cuts)], refs[-1]
    me = lax.axis_index("dp") // PAIR
    for k in range(count):
        held[came_from(me, k, count)] = ins[k][...]
    for out, (low, high, rows) in zip(outs, cuts):
        q = high - low
        for g in range(count):
            n = max(0, min(q, rows - g * q))
            if n and len(ins[0].shape) == 3:
                out[:, g * q : g * q + n, :] = held[g, :, low : low + n, :]
            elif n and len(out.shape) == 3:
                out[0, g * q : g * q + n, :] = held[g, low : low + n, :].astype(out.dtype)
            elif n:
                out[g * q : g * q + n, :] = held[g, low : low + n, :].astype(out.dtype)


def join_rows(pieces, cuts, dtype=BF16, lead=()):
    count = len(pieces)
    shape = pieces[0].shape
    return call(
        functools.partial(join_body, count, cuts),
        [(lead + (rows, shape[-1]), dtype) for _, _, rows in cuts],
        [VM] * count,
        pieces,
        [pltpu.VMEM((count,) + shape, BF16)],
    )


def holds(tp, i, j):
    if tp != 4:
        return i - j if i >= j else tp - 1 + j - i
    return i ^ j if i ^ j < 3 else 3 + int(i in (0, tp - 1))


def block_count(tp):
    return 5 if tp == 4 else 2 * tp - 1


def chain_gather(block, axis):
    tp = lax.axis_size(axis)

    def move(value, pairs):
        return lax.ppermute(value, axis, pairs)

    if tp == 4:
        far = move(block, [(i, i ^ 2) for i in range(4)])
        pair = move(block, [(i, i ^ 1) for i in range(4)])
        mid = move(block, [(1, 2), (2, 1)])
        passed = move(far, [(1, 0), (2, 3)])
        return [block, pair, far, mid, passed]
    from_left, from_right = [block], [block]
    for hop in range(1, tp):
        right = [(i, i + 1) for i in range(hop - 1, tp - 1)]
        left = [(i, i - 1) for i in range(1, tp - hop + 1)]
        from_left.append(move(from_left[-1], right))
        from_right.append(move(from_right[-1], left))
    return [block, *from_left[1:], *from_right[1:]]


def spin(x, cosine, sine):
    return x * cosine + pltpu.roll(x, HD // 2, 1) * sine


def nt(a, b):
    return lax.dot_general(a, b, (((1,), (1,)), ((), ())), preferred_element_type=F32)


def tn(a, b):
    return lax.dot_general(a, b, (((0,), (0,)), ((), ())), preferred_element_type=F32)


def chunk_body(cfg, *refs):
    refs = list(refs)

    def take(n):
        out = refs[:n]
        del refs[:n]
        return out

    tp, first, last = cfg["tp"], cfg["first"], cfg["last"]
    rows, lead, lead_pad = cfg["rows"], cfg["lead"], cfg["lead_pad"]
    prompt_len, keys_pad, start = cfg["prompt_len"], cfg["keys_pad"], cfg["start"]
    width, heads, prior = cfg["width"], cfg["heads"], cfg["prior"]
    depth, cols = tp * width, heads * HD
    slot, lengths, gain = take(3)
    weights = take(3)
    cosine, sine, cot = take(3)
    segments = [take(block_count(tp) if chained else 1) for chained, _ in cfg["segments"]]
    before = [take(2) for _ in prior]
    if not first:
        gk_in, gv_in = take(2)
    if last:
        inv_lead, flat_lead, dot_lead = take(3)
    (out,) = take(1)
    if last:
        turned, pull_out = take(2)
    else:
        k_out, v_out, gk_out, gv_out = take(4)
        if first:
            x_out, inv_out, flat_out, dot_out, turned = take(5)
    x_buf, n_buf, acc, k_all, v_all = take(5)
    if last:
        gk_out, gv_out = take(2)

    def weight(m, j):
        return weights[m][pl.ds(pl.multiple_of(j * width, width), width), :]

    at = 0
    for blocks, (chained, n) in zip(segments, cfg["segments"]):
        if chained:
            gather_blocks(tp, blocks, x_buf, at)
        else:
            x_buf[:, at : at + n, :] = blocks[0][...]
        at += n
    square = jnp.zeros((rows, 1), F32)
    for j in range(tp):
        wide = x_buf[j].astype(F32)
        square = square + jnp.sum(wide * wide, axis=1, keepdims=True)
    inv_rms = lax.rsqrt(square / depth + 1e-05)
    for j in range(tp):
        n_buf[j] = (x_buf[j].astype(F32) * inv_rms * gain[j]).astype(BF16)
    if first:
        x_out[...] = x_buf[:, :lead, :]
        inv_out[...] = jnp.broadcast_to(inv_rms[:lead], (lead, HD))
    acc[...] = jnp.zeros_like(acc)

    def project(j, _):
        for m in range(3):
            acc[m] += jnp.dot(n_buf[j], weight(m, j), preferred_element_type=F32)
        return 0

    lax.fori_loop(0, tp, project, 0)
    length = find(slot, lengths, lax.axis_index("dp"), cfg["examples"])
    limit = lead + length
    at = 0
    for (k_ref, v_ref), n in zip(before, prior):
        k_all[at : at + n, :] = k_ref[...]
        v_all[at : at + n, :] = v_ref[...]
        at += n
    if keys_pad > at + rows:
        k_all[at + rows :, :] = jnp.zeros((keys_pad - at - rows, cols), BF16)
        v_all[at + rows :, :] = jnp.zeros((keys_pad - at - rows, cols), BF16)
    cos, sin = cosine[start : start + rows, :], sine[start : start + rows, :]
    scale = 1.0 / math.sqrt(HD)
    r = lax.broadcasted_iota(jnp.int32, (rows, keys_pad), 0) + start
    c = lax.broadcasted_iota(jnp.int32, (rows, keys_pad), 1)
    allowed = (c <= r) & ((c < prompt_len) | (c >= lead)) & (c < limit)
    live = lax.broadcasted_iota(jnp.int32, (rows, HD), 0) + start < limit
    dot = jnp.zeros((rows, 1), F32)
    for h in range(heads):
        s = slice(h * HD, (h + 1) * HD)
        q = spin(acc[0, :, s], cos, sin).astype(BF16)
        k_all[at : at + rows, s] = spin(acc[1, :, s], cos, sin).astype(BF16)
        v_all[at : at + rows, s] = acc[2, :, s].astype(BF16)
        k, v = k_all[:, s], v_all[:, s]
        scores = jnp.where(allowed, nt(q, k) * scale, -1e30)
        peak = jnp.max(scores, axis=1, keepdims=True)
        w = jnp.exp(scores - peak)
        prob = w * (1.0 / jnp.sum(w, axis=1, keepdims=True))
        low = prob.astype(BF16)
        mixed = jnp.dot(low, v, preferred_element_type=F32)
        out[:, s] = jnp.where(live, mixed, 0.0).astype(BF16)
        up = jnp.where(live, cot[:, s].astype(F32), 0.0).astype(BF16)
        grad_prob = nt(up, v)
        delta = jnp.sum(prob * grad_prob, axis=1, keepdims=True)
        score = (prob * (grad_prob - delta)).astype(BF16)
        gk = tn(score[:, :lead_pad], q)
        gv = tn(low[:, :lead_pad], up)
        if first:
            gk_out[:, s] = gk
            gv_out[:, s] = gv
            gq = jnp.dot(score, k, preferred_element_type=F32) * scale
            gq = spin(gq, cos, -sin).astype(BF16).astype(F32)
            dot = dot + jnp.sum(gq * acc[0, :, s], axis=1, keepdims=True)
            gq = jnp.concatenate([gq, jnp.zeros((lead_pad - lead, HD), F32)], axis=0)
            turned[s, :] = gq.T.astype(BF16)
        else:
            gk_out[:, s] = gk_in[:, s] + gk
            gv_out[:, s] = gv_in[:, s] + gv
    if first:
        flat_out[...] = acc[1:]
        dot_out[...] = jnp.broadcast_to(dot, (rows, HD))
    if not last:
        k_out[...] = k_all[at : at + rows, :]
        v_out[...] = v_all[at : at + rows, :]
        return
    cos, sin = cosine[:lead_pad, :], sine[:lead_pad, :]
    dot = dot_lead[:, :1]
    for h in range(heads):
        s = slice(h * HD, (h + 1) * HD)
        gk = spin(gk_out[:, s] * scale, cos, -sin).astype(BF16).astype(F32)
        gv = gv_out[:, s].astype(BF16).astype(F32)
        dot = dot + jnp.sum(gk[:lead] * flat_lead[0, :, s], axis=1, keepdims=True)
        dot = dot + jnp.sum(gv[:lead] * flat_lead[1, :, s], axis=1, keepdims=True)
        turned[0, s, :] = gk.T.astype(BF16)
        turned[1, s, :] = gv.T.astype(BF16)
    inv = inv_lead[:, :1]
    pull_out[...] = jnp.broadcast_to(inv * inv * (dot / depth), (lead, HD))


def back_body(tp, k, gain, wq, wk, wv, x_lead, inv_lead, pull, turned_q, turned, out):
    lead, width = out.shape
    to = partner(lax.axis_index("tensor"), k, tp)
    at = pl.ds(pl.multiple_of(to * width, width), width)
    gn = jnp.dot(wq[at, :], turned_q[...], preferred_element_type=F32)
    gn = gn + jnp.dot(wk[at, :], turned[0], preferred_element_type=F32)
    gn = gn + jnp.dot(wv[at, :], turned[1], preferred_element_type=F32)
    gn = gn.T[:lead] * gain[to]
    out[...] = (inv_lead[:, :1] * gn - x_lead[to].astype(F32) * pull[:, :1]).astype(BF16)


def stack_body(lead_rows, *refs):
    out, at = refs[-1], 0
    for i, part in enumerate(refs[:-1]):
        n = part.shape[0] if i else lead_rows
        out[0, at : at + n, :] = part[:n, :]
        at += n


def sum_body(count, n, *refs):
    ins, outs, whole, held = refs[:n], refs[n : n + count], refs[n + count], refs[n + count + 1]
    rows, q = ins[0].shape[0], outs[0].shape[0]
    total = ins[0][...].astype(F32)
    for i in range(1, n):
        total = total + ins[i][...].astype(F32)
    whole[...] = total.astype(BF16)
    for g in range(count):
        m = max(0, min(q, rows - g * q))
        if m < q:
            held[g] = jnp.zeros(held.shape[1:], BF16)
        if m:
            held[g, :m, :] = whole[g * q : g * q + m, :]
    me = lax.axis_index("dp") // PAIR
    for k in range(count):
        outs[k][...] = held[partner(me, k, count)]


def collect_body(count, examples, slot, task_of, *refs):
    ins, mine, other = refs[:count], refs[count], refs[count + 1]
    index = lax.axis_index("dp")
    me, core = index // PAIR, lax.rem(index, PAIR)
    tasks = []
    for k in range(count):
        place = came_from(me, k, count) * PAIR + core
        tasks.append(find(slot, task_of, place, examples))
    for g in range(count):
        for target, side in ((mine, core), (other, 1 - core)):
            total = jnp.zeros(ins[0].shape, F32)
            for k in range(count):
                share = jnp.where(tasks[k] == g * PAIR + side, 1.0, 0.0)
                total = total + share * ins[k][...].astype(F32)
            target[g] = total.astype(target.dtype)


def finish_body(count, mine, other, *outs):
    me = lax.axis_index("dp") // PAIR
    for k in range(count):
        p = partner(me, k, count)
        outs[k][...] = (mine[p] + other[p].astype(F32)).astype(BF16)


def on_device(text, prompts, gain, w_query, w_key, w_value, cotangent, task_of, lengths, slot):
    count = lax.axis_size("dp") // PAIR
    tp = lax.axis_size("tensor")
    prompt_len, text_len, width = prompts.shape[1], text.shape[1], text.shape[2]
    examples = slot.shape[0]
    cols = w_query.shape[1]
    heads = cols // HD
    lead = up_to(prompt_len, 8)
    lead_pad = up_to(lead, 128)
    early = text_len // 2
    late = text_len - early
    prompt_q = up_to(-(-prompt_len // count), 16)
    late_q, early_q = late // count, early // count
    wide = chain_gather(text[0, :early], "tensor")
    piece = (prompt_q + late_q, width)
    pieces = call(
        functools.partial(split_body, count, prompt_q, early),
        [(piece, BF16)] * count,
        [VM, VM],
        [prompts, text],
        [pltpu.VMEM((count,) + piece, BF16)],
    )
    placed = place_rows(pieces, slot, task_of, prompt_q)
    cuts = [(0, prompt_q, lead), (prompt_q, prompt_q + late_q, late)]
    rows_a, rows_c = join_rows(placed, cuts)
    chain_a = chain_gather(rows_a, "tensor")
    chain_c = chain_gather(rows_c, "tensor")
    wide_pieces = call(
        functools.partial(spread_body, count, tp),
        [((tp, early_q, width), BF16)] * count,
        [VM] * len(wide),
        wide,
        [pltpu.VMEM((tp, early, width), BF16)],
    )
    wide_placed = place_rows(wide_pieces, slot, task_of, 0)
    (rows_b,) = join_rows(wide_placed, [(0, early_q, early)], BF16, (tp,))

    at = jnp.arange(lead + text_len, dtype=jnp.int32)
    at = jnp.where(at < lead, at, at - (lead - prompt_len)).astype(F32)
    frequency = 10000.0 ** (-jnp.arange(HD // 2, dtype=F32) / (HD // 2))
    angle = at[:, None] * frequency[None, :]
    cosine, sine = jnp.cos(angle), jnp.sin(angle)
    cosine = jnp.concatenate([cosine, cosine], axis=1)
    sine = jnp.concatenate([-sine, sine], axis=1)
    gain_rows = gain.reshape(tp, 1, width)
    split_at = prompt_len + early
    cots = [
        jnp.pad(cotangent[0, :prompt_len], ((0, lead - prompt_len), (0, 0))),
        cotangent[0, prompt_len:split_at],
        cotangent[0, split_at:],
    ]
    chunks = [
        ([(True, lead)], chain_a),
        ([(False, early)], [rows_b]),
        ([(True, late)], chain_c),
    ]
    outputs, before, grads, saved, start = [], [], [], [], 0
    for i, (segments, blocks) in enumerate(chunks):
        first, last = i == 0, i == len(chunks) - 1
        rows = cots[i].shape[0]
        keys_pad = up_to(start + rows, 128)
        cfg = dict(
            tp=tp, first=first, last=last, rows=rows, lead=lead, lead_pad=lead_pad,
            prompt_len=prompt_len, keys_pad=keys_pad, start=start, width=width, heads=heads,
            prior=[k.shape[0] for k, _ in before], examples=examples, segments=segments,
        )
        args = [slot, lengths, gain_rows, w_query, w_key, w_value, cosine, sine, cots[i]]
        specs = [SM, SM] + [VM] * 7
        extra = list(blocks)
        for pair in before:
            extra += pair
        extra += grads + (saved[1:4] if last else [])
        outs = [((rows, cols), BF16)]
        scratch = [
            pltpu.VMEM((tp, rows, width), BF16),
            pltpu.VMEM((tp, rows, width), BF16),
            pltpu.VMEM((3, rows, cols), F32),
            pltpu.VMEM((keys_pad, cols), BF16),
            pltpu.VMEM((keys_pad, cols), BF16),
        ]
        if last:
            outs += [((2, cols, lead_pad), BF16), ((lead, HD), F32)]
            scratch += [pltpu.VMEM((lead_pad, cols), F32)] * 2
        else:
            outs += [((rows, cols), BF16)] * 2 + [((lead_pad, cols), F32)] * 2
            if first:
                outs += [((tp, lead, width), BF16), ((lead, HD), F32), ((2, lead, cols), F32)]
                outs += [((lead, HD), F32), ((cols, lead_pad), BF16)]
        got = call(
            functools.partial(chunk_body, cfg),
            outs,
            specs + [VM] * len(extra),
            args + extra,
            scratch,
            flops=2 * rows * tp * width * 3 * cols,
        )
        outputs.append(got[0])
        if last:
            turned, pull = got[1:]
        else:
            before.append((got[1], got[2]))
            grads = [got[3], got[4]]
            if first:
                saved = list(got[5:])
        start += rows

    x_lead, inv_lead, _, _, turned_q = saved
    got = []
    for k in reversed(range(tp)):
        (block,) = call(
            functools.partial(back_body, tp, k),
            [((lead, width), BF16)],
            [VM] * 9,
            [gain_rows, w_query, w_key, w_value, x_lead, inv_lead, pull, turned_q, turned],
        )
        if k:
            pairs = [(i, i ^ k if tp & (tp - 1) == 0 else (i + k) % tp) for i in range(tp)]
            block = lax.ppermute(block, "tensor", pairs)
        got.append(block)
    (output,) = call(
        functools.partial(stack_body, prompt_len),
        [((1, prompt_len + text_len, cols), BF16)],
        [VM] * len(outputs),
        outputs,
    )
    pieces = call(
        functools.partial(sum_body, count, tp),
        [((prompt_q, width), BF16)] * count,
        [VM] * tp,
        got,
        [pltpu.VMEM((lead, width), BF16), pltpu.VMEM((count, prompt_q, width), BF16)],
    )
    mine, other = call(
        functools.partial(collect_body, count, examples),
        [((count, prompt_q, width), F32), ((count, prompt_q, width), BF16)],
        [SM, SM] + [VM] * count,
        [slot, task_of, *to_groups(pieces)],
    )
    done = call(
        functools.partial(finish_body, count),
        [((prompt_q, width), BF16)] * count,
        [VM, VM],
        [mine, to_sibling(other)],
    )
    (prompt_grad,) = join_rows(to_groups(done), [(0, prompt_q, prompt_len)], F32, (1,))
    return (output, prompt_grad)


def solution(mesh):
    in_specs = (
        P("dp", None, "tensor"),
        P("dp", None, "tensor"),
        P(),
        P(None, "tensor"),
        P(None, "tensor"),
        P(None, "tensor"),
        P("dp", None, "tensor"),
        P(),
        P(),
        P(),
    )
    out_specs = (P("dp", None, "tensor"), P("dp", None, "tensor"))
    return jax.shard_map(
        on_device, mesh=mesh, in_specs=in_specs, out_specs=out_specs, check_vma=False
    )
```
